256 devices in a mesh: items: 4 (over x), users: 64 (over z, y, core).
Axes of the slice: x: 4, y: 4, z: 8, core: 2. Of those that a mesh axis runs over, the one named last changes fastest.
Arguments:
- capsules: bfloat16 [4096, 8, 128], P('users'), may hold values from -6 to 6
- bank: bfloat16 [262144, 128], P(('items', 'users')), may hold values from -0.5 to 0.5
Outputs:
- relative: float32 [4096, 256], P('users', 'items')
- peak: float32 [4096], P('users')
The draws below stay inside these ranges and needn't reach their ends.
All inputs are finite; a program needn't handle non-finite values.
Results may differ from the reference program's by a relative error of at most 0.0003.
Values may be sent and summed in bfloat16 or wider, within the bound.
No kernel may reach another device: no remote copies, remote signals or barrier semaphores. Data moves between devices by JAX's collectives and lax.ppermute only.
A program may use at most 64 MiB of HBM per device.

```python
import jax
import jax.numpy as jnp
from jax import lax

E = 128
K = 8
BLOCK = 1024
USERS = 4096
NB = 256
NITEMS = 262144


def block_levels(key, shape, split, least, largest):
    gain, own = 1.0, jax.random.fold_in(key, 6)
    for axis_at, shards_of in split:
        steps = jnp.exp(jax.random.uniform(jax.random.fold_in(own, axis_at), (shards_of,), jnp.float32, least / len(split), largest / len(split)))
        gain = gain * jnp.repeat(steps, shape[axis_at] // shards_of).reshape([-1 if axis == axis_at else 1 for axis in range(len(shape))])
    return gain


def normal_values(key, shape, scale, limit, split=(), kind=jnp.bfloat16):
    array = scale * jax.random.normal(key, shape, jnp.float32)
    if split:
        array = array * block_levels(key, shape, split, -0.22, 0.18)
    return jnp.clip(array, -limit, limit).astype(kind)


def setup_inputs(seed: int = 0) -> dict:
    streams_of = jax.random.split(jax.random.key(seed), 3)
    capsules = normal_values(streams_of[0], (USERS, K, E), 1.0, 6.0, ((0, 64),))
    bank = normal_values(streams_of[1], (NITEMS, E), E ** -0.5, 0.5, ((0, 256),))
    return {"capsules": capsules, "bank": bank}


def reference(capsules, bank):
    flat = capsules.reshape(USERS * K, E)
    blocks = bank.reshape(NB, BLOCK, E)

    def one_block(rows):
        score = jnp.dot(flat, rows.T, preferred_element_type=jnp.float32)
        return jnp.max(score.reshape(USERS, K * BLOCK), axis=1)

    block_peak = lax.map(one_block, blocks).T
    peak = jnp.max(block_peak, axis=1)
    return block_peak - peak[:, None], peak
```

```python
import jax
import jax.numpy as jnp
from jax import lax
from jax.experimental import pallas as pl
from jax.experimental.pallas import tpu as pltpu
from jax.sharding import Mesh, PartitionSpec as P

BLOCK = 1024
AXES = ("x", "z", "y", "c")
SIZES = (4, 8, 4, 2)
NEG = float("-inf")
LIMIT = 16 << 20
VMEM = pl.BlockSpec(memory_space=pltpu.VMEM)


def flat(x, z, y, c):
    return ((x * SIZES[1] + z) * SIZES[2] + y) * SIZES[3] + c


def move(value, target):
    pairs = []
    for x in range(SIZES[0]):
        for z in range(SIZES[1]):
            for y in range(SIZES[2]):
                for c in range(SIZES[3]):
                    pairs.append((flat(x, z, y, c), flat(*target(x, z, y, c))))
    return lax.ppermute(value, AXES, pairs)


def along(c):
    return 2 * c - 1


def to_partner(value):
    return move(value, lambda x, z, y, c: (x, z, y, 1 - c))


def down_z(value):
    return move(value, lambda x, z, y, c: (x, (z - along(c)) % SIZES[1], y, c))


def down_y(value):
    return move(value, lambda x, z, y, c: (x, z, (y - along(c)) % SIZES[2], c))


def score_rows(caps, items):
    flat_caps = caps
    best = None
    for at in range(0, BLOCK, 256):
        score = lax.dot_general(
            items[at : at + 256], flat_caps, (((1,), (1,)), ((), ())),
            preferred_element_type=jnp.float32,
        )
        part = jnp.max(score.reshape(32, 8, 512), axis=0)
        best = part if best is None else jnp.maximum(best, part)
    return jnp.max(best, axis=0, keepdims=True)


def pieces(refs, height):
    return [(r, at) for r in refs for at in range(0, r.shape[0], height)]


def scores(groups, blocks):
    n_groups, n_blocks = len(groups), len(blocks)

    def body(*refs):
        out = refs[-1]
        caps = pieces(refs[:n_groups], 512)
        items = pieces(refs[n_groups:-1], BLOCK)
        for g, (cref, cat) in enumerate(caps):
            own = cref[cat : cat + 512, :]
            for b, (iref, iat) in enumerate(items):
                out[pl.ds(g * len(items) + b, 1), :] = score_rows(own, iref.at[iat : iat + BLOCK, :])

    rows = sum(v.shape[0] // 512 for v in groups) * sum(v.shape[0] // BLOCK for v in blocks)
    return pl.pallas_call(
        body,
        out_shape=jax.ShapeDtypeStruct((rows, 512), jnp.float32),
        in_specs=[VMEM] * (n_groups + n_blocks),
        out_specs=VMEM,
        compiler_params=pltpu.CompilerParams(vmem_limit_bytes=LIMIT),
        cost_estimate=pl.CostEstimate(
            flops=rows * 2 * 512 * BLOCK * 128 * 2, bytes_accessed=1 << 16, transcendentals=0
        ),
    )(*groups, *blocks)


def gather_rows(parts, places):
    def body(*refs):
        out, rows = refs[-2], refs[-1]
        z = lax.axis_index("z")
        y = lax.axis_index("y")
        c = lax.axis_index("c")
        step = 2 * c - 1
        for ref, place in zip(refs, places):
            for r, (group, (dy, other)) in enumerate(place):
                at_y = (y + step * dy + 4) % 4
                at_c = 1 - c if other else c
                rows[pl.ds(group * 8 + at_y * 2 + at_c, 1), :] = ref[r : r + 1, :]
        by_capsule = rows[...].T
        by_user = jnp.max(by_capsule.reshape(64, 8, 64), axis=1)
        peaks = jnp.concatenate([by_user, jnp.zeros((64, 64), jnp.float32)], axis=0).T
        out[...] = jnp.full(out.shape, NEG, jnp.float32)
        for group, (dz, other) in enumerate(GROUPS):
            at_z = (z + step * dz + 8) % 8
            at_c = 1 - c if other else c
            for x in range(4):
                out[x * 16 + at_z * 2 + at_c] = peaks[group * 8 : group * 8 + 8, :]

    return pl.pallas_call(
        body,
        out_shape=jax.ShapeDtypeStruct((64, 8, 128), jnp.float32),
        in_specs=[VMEM] * len(parts),
        out_specs=VMEM,
        compiler_params=pltpu.CompilerParams(vmem_limit_bytes=LIMIT),
        scratch_shapes=[pltpu.VMEM((64, 512), jnp.float32)],
    )(*parts)


GROUPS = [(0, 0), (1, 0), (1, 1), (2, 0), (2, 1), (3, 0), (3, 1), (4, 0)]


def finish(table):
    def body(table_ref, relative, peak):
        x = lax.axis_index("x")
        best = jnp.max(table_ref[...], axis=0)
        top = jnp.max(best, axis=0, keepdims=True)
        mine = jnp.concatenate(
            [jnp.maximum(table_ref[x * 16 + 2 * z], table_ref[x * 16 + 2 * z + 1]) for z in range(8)], axis=0
        )
        relative[...] = (mine - top).T[:64, :]
        peak[...] = top[0, :64]

    return pl.pallas_call(
        body,
        out_shape=(jax.ShapeDtypeStruct((64, 64), jnp.float32), jax.ShapeDtypeStruct((64,), jnp.float32)),
        in_specs=[VMEM],
        compiler_params=pltpu.CompilerParams(vmem_limit_bytes=LIMIT),
        out_specs=(VMEM, VMEM),
    )(table)


def per_device(capsules, bank):
    own = capsules.reshape(512, 128)
    own_pair = jnp.concatenate([own, to_partner(own)], axis=0)
    block_pair = jnp.concatenate([bank, to_partner(bank)], axis=0)
    z1 = down_z(own_pair)
    z2 = down_z(z1)
    z3 = down_z(z2)
    z4 = down_z(z3[:512])
    y1 = down_y(block_pair)
    y2 = down_y(y1[:BLOCK])
    y1x = to_partner(y1)
    y2x = to_partner(y2)
    b0 = [(0, 0), (0, 1)]
    b1 = [(1, 0), (1, 1)]
    b1x = [(-1, 1), (-1, 0)]
    b2 = [(2, 0)]
    b2x = [(2, 1)]

    plan = [
        ([own], [0], [block_pair], b0),
        ([z1], [1, 2], [block_pair], b0),
        ([own, z1], [0, 1, 2], [y1], b1),
        ([own, z1], [0, 1, 2], [y1x], b1x),
        ([z2], [3, 4], [block_pair, y1, y1x], b0 + b1 + b1x),
        ([own, z1, z2], [0, 1, 2, 3, 4], [y2, y2x], b2 + b2x),
        ([z3], [5, 6], [block_pair, y1, y1x, y2, y2x], b0 + b1 + b1x + b2 + b2x),
        ([z4], [7], [block_pair, y1, y1x, y2, y2x], b0 + b1 + b1x + b2 + b2x),
    ]
    parts, places = [], []
    for groups, ids, blocks, names in plan:
        parts.append(scores(groups, blocks))
        places.append([(g, b) for g in ids for b in names])
    ready = gather_rows(parts, places)
    table = lax.all_to_all(ready, ("x", "z", "c"), 0, 0, tiled=True)
    return finish(table)


def solution(mesh):
    grid = Mesh(mesh.devices.reshape(SIZES), AXES)
    return jax.shard_map(
        per_device,
        mesh=grid,
        in_specs=(P(("z", "y", "c"), None, None), P(AXES, None)),
        out_specs=(P(("z", "y", "c"), "x"), P(("z", "y", "c"))),
        check_vma=False,
    )
```

```python
import jax
import jax.numpy as jnp
from jax import lax
from jax.experimental import pallas as pl
from jax.experimental.pallas import tpu as pltpu
from jax.sharding import Mesh, PartitionSpec as P

BLOCK = 1024
AXES = ("x", "z", "y", "c")
SIZES = (4, 8, 4, 2)
LIMIT = 16 << 20
VMEM = pl.BlockSpec(memory_space=pltpu.VMEM)
KEPT = [(0, 0), (1, 0), (2, 0), (3, 0), (4, 0)]
SWAPPED = [(1, 1), (2, 1), (3, 1)]


def flat(x, z, y, c):
    return ((x * SIZES[1] + z) * SIZES[2] + y) * SIZES[3] + c


def move(value, target):
    pairs = []
    for x in range(SIZES[0]):
        for z in range(SIZES[1]):
            for y in range(SIZES[2]):
                for c in range(SIZES[3]):
                    pairs.append((flat(x, z, y, c), flat(*target(x, z, y, c))))
    return lax.ppermute(value, AXES, pairs)


def along(c):
    return 2 * c - 1


def to_partner(value):
    return move(value, lambda x, z, y, c: (x, z, y, 1 - c))


def down_z(value, steps=1):
    return move(value, lambda x, z, y, c: (x, (z - steps * along(c)) % SIZES[1], y, c))


def down_y(value, steps=1):
    return move(value, lambda x, z, y, c: (x, z, (y - steps * along(c)) % SIZES[2], c))


def after(value, *earlier):
    return lax.optimization_barrier((value, *earlier))[0]


def score_row(caps, items):
    best = None
    for at in range(0, BLOCK, 256):
        score = lax.dot_general(
            items[at : at + 256], caps, (((1,), (1,)), ((), ())),
            preferred_element_type=jnp.float32,
        )
        part = jnp.max(score.reshape(32, 8, 512), axis=0)
        best = part if best is None else jnp.maximum(best, part)
    return jnp.max(best, axis=0, keepdims=True)


def pieces(refs, height):
    return [r.at[at : at + height, :] for r in refs for at in range(0, r.shape[0], height)]


def scores(groups, blocks):
    n = len(groups)

    def body(*refs):
        out = refs[-1]
        items = pieces(refs[n:-1], BLOCK)
        for g, cref in enumerate(pieces(refs[:n], 512)):
            own = cref[...]
            for b, iref in enumerate(items):
                out[pl.ds(g * len(items) + b, 1), :] = score_row(own, iref)

    rows = sum(v.shape[0] // 512 for v in groups) * sum(v.shape[0] // BLOCK for v in blocks)
    return pl.pallas_call(
        body,
        out_shape=jax.ShapeDtypeStruct((rows, 512), jnp.float32),
        in_specs=[VMEM] * (n + len(blocks)),
        out_specs=VMEM,
        compiler_params=pltpu.CompilerParams(vmem_limit_bytes=LIMIT),
        cost_estimate=pl.CostEstimate(
            flops=rows * 2 * 512 * BLOCK * 128 * 2, bytes_accessed=1 << 16, transcendentals=0
        ),
    )(*groups, *blocks)


def user_rows(parts, groups):
    n = len(groups)
    used = [(v, names) for v, names in parts if any(name and name[0] in groups for name in names)]

    def body(*refs):
        out, rows = refs[-2], refs[-1]
        y = lax.axis_index("y")
        c = lax.axis_index("c")
        for ref, (_, names) in zip(refs, used):
            for r, (group, (dy, other)) in enumerate(names):
                if group in groups:
                    at = ((y + along(c) * dy + 4) % 4) * 2 + (1 - c if other else c)
                    place = (at // 4) * (4 * n) + groups.index(group) * 4 + at % 4
                    rows[pl.ds(place, 1), :] = ref[r : r + 1, :]
        by_user = jnp.max(rows[...].T.reshape(64, 8, 8 * n), axis=1)
        halves = jnp.concatenate([by_user[:, : 4 * n], by_user[:, 4 * n :]], axis=0)
        out[...] = halves.T.reshape(n, 4, 128)

    return pl.pallas_call(
        body,
        out_shape=jax.ShapeDtypeStruct((n, 4, 128), jnp.float32),
        in_specs=[VMEM] * len(used),
        out_specs=VMEM,
        compiler_params=pltpu.CompilerParams(vmem_limit_bytes=LIMIT),
        scratch_shapes=[pltpu.VMEM((8 * n, 512), jnp.float32)],
    )(*[v for v, _ in used])


def by_owner(kept, swapped):
    def body(kept_ref, swapped_ref, out):
        z = lax.axis_index("z")
        step = along(lax.axis_index("c"))
        for x in range(SIZES[0]):
            for i, (dz, _) in enumerate(KEPT):
                out[x * 8 + (z + step * dz + 8) % 8] = kept_ref[i]
            for i, (dz, _) in enumerate(SWAPPED):
                out[x * 8 + (z - step * dz + 8) % 8] = swapped_ref[i]

    return pl.pallas_call(
        body,
        out_shape=jax.ShapeDtypeStruct((32, 4, 128), jnp.float32),
        in_specs=[VMEM, VMEM],
        out_specs=VMEM,
        compiler_params=pltpu.CompilerParams(vmem_limit_bytes=LIMIT),
    )(kept, swapped)


def finish(table):
    def body(table_ref, relative, peak):
        x = lax.axis_index("x")
        top = jnp.max(jnp.max(table_ref[...], axis=0), axis=0, keepdims=True)
        top = jnp.maximum(top[:, :64], top[:, 64:])
        mine = [table_ref[x * 8 + z] for z in range(8)]
        rows = jnp.concatenate([part for m in mine for part in (m[:, :64], m[:, 64:])], axis=0)
        relative[...] = (rows - top).T
        peak[...] = top[0]

    return pl.pallas_call(
        body,
        out_shape=(jax.ShapeDtypeStruct((64, 64), jnp.float32), jax.ShapeDtypeStruct((64,), jnp.float32)),
        in_specs=[VMEM],
        out_specs=(VMEM, VMEM),
        compiler_params=pltpu.CompilerParams(vmem_limit_bytes=LIMIT),
    )(table)


def peaks(capsules, bank):
    own = capsules.reshape(512, 128)
    own_x = to_partner(own)
    bank_x = to_partner(bank)
    own_pair = jnp.concatenate([own, own_x], axis=0)
    block_pair = jnp.concatenate([bank, bank_x], axis=0)
    here, ahead, behind, far, far_x = [(0, 0), (0, 1)], [(1, 0), (1, 1)], [(-1, 1), (-1, 0)], [(2, 0)], [(2, 1)]
    g0, g1, g2, g3, g4 = [(0, 0)], [(1, 0), (1, 1)], [(2, 0), (2, 1)], [(3, 0), (3, 1)], [(4, 0)]
    parts = []

    def score(caps, groups, items, blocks):
        parts.append((scores(caps, items), [(g, b) for g in groups for b in blocks]))

    z1 = down_z(own_pair)
    y1 = down_y(block_pair)
    z2 = down_z(own_pair, 2)
    y2 = down_y(y1[:BLOCK])
    z3 = down_z(z1, 2)
    y1x = to_partner(y1)
    y2x = to_partner(y2)
    score([own], g0, [block_pair], here)
    score([z1], g1, [block_pair], here)
    score([own, z1], g0 + g1, [y1], ahead)
    score([own, z1], g0 + g1, [y1x], behind)
    score([z2], g2, [block_pair, y1, y1x], here + ahead + behind)
    far_half = after(z3, parts[-1][0])[:512]
    z4 = down_z(far_half)
    score([z3], g3, [block_pair, y1, y1x], here + ahead + behind)
    score([own, z1, z2, z3], g0 + g1 + g2 + g3, [y2, y2x], far + far_x)
    rows = user_rows(parts, SWAPPED)
    swapped = to_partner(rows)
    score([z4], g4, [block_pair, y1, y1x, y2, y2x], here + ahead + behind + far + far_x)
    table = lax.all_to_all(by_owner(user_rows(parts, KEPT), swapped), ("x", "z"), 0, 0, tiled=True)
    return finish(table)


def solution(mesh):
    grid = Mesh(mesh.devices.reshape(SIZES), AXES)
    return jax.shard_map(
        peaks,
        mesh=grid,
        in_specs=(P(("z", "y", "c"), None, None), P(AXES, None)),
        out_specs=(P(("z", "y", "c"), "x"), P(("z", "y", "c"))),
        check_vma=False,
    )
```

```python
import jax
import jax.numpy as jnp
from jax import lax
from jax.experimental import pallas as pl
from jax.experimental.pallas import tpu as pltpu
from jax.sharding import Mesh, PartitionSpec as P

BLOCK = 1024
AXES = ("x", "z", "y", "c")
SIZES = (4, 8, 4, 2)
LIMIT = 16 << 20
VMEM = pl.BlockSpec(memory_space=pltpu.VMEM)
KEPT = [(0, 0), (1, 0), (2, 0), (3, 0), (4, 0)]
SWAPPED = [(1, 1), (2, 1), (3, 1)]


def flat(x, z, y, c):
    return ((x * SIZES[1] + z) * SIZES[2] + y) * SIZES[3] + c


def move(value, target):
    pairs = []
    for x in range(SIZES[0]):
        for z in range(SIZES[1]):
            for y in range(SIZES[2]):
                for c in range(SIZES[3]):
                    pairs.append((flat(x, z, y, c), flat(*target(x, z, y, c))))
    return lax.ppermute(value, AXES, pairs)


def along(c):
    return 2 * c - 1


def to_partner(value):
    return move(value, lambda x, z, y, c: (x, z, y, 1 - c))


def down_z(value, steps=1):
    return move(value, lambda x, z, y, c: (x, (z - steps * along(c)) % SIZES[1], y, c))


def down_y(value, steps=1):
    return move(value, lambda x, z, y, c: (x, z, (y - steps * along(c)) % SIZES[2], c))


def after(value, *earlier):
    return lax.optimization_barrier((value, *earlier))[0]


def score_row(caps, items):
    best = None
    for at in range(0, BLOCK, 256):
        score = lax.dot_general(
            items[at : at + 256], caps, (((1,), (1,)), ((), ())),
            preferred_element_type=jnp.float32,
        )
        part = jnp.max(score.reshape(32, 8, 512), axis=0)
        best = part if best is None else jnp.maximum(best, part)
    return jnp.max(best, axis=0, keepdims=True)


def pieces(refs, height):
    return [r.at[at : at + height, :] for r in refs for at in range(0, r.shape[0], height)]


def scores(*jobs):
    arrays = []
    for groups, blocks in jobs:
        for v in groups + blocks:
            if not any(v is w for w in arrays):
                arrays.append(v)

    def body(*refs):
        ref_of = lambda v: next(r for r, w in zip(refs, arrays) if w is v)
        for (groups, blocks), out in zip(jobs, refs[len(arrays):]):
            items = pieces([ref_of(v) for v in blocks], BLOCK)
            for g, cref in enumerate(pieces([ref_of(v) for v in groups], 512)):
                own = cref[...]
                for b, iref in enumerate(items):
                    out[pl.ds(g * len(items) + b, 1), :] = score_row(own, iref)

    rows = [sum(v.shape[0] // 512 for v in g) * sum(v.shape[0] // BLOCK for v in b) for g, b in jobs]
    return pl.pallas_call(
        body,
        out_shape=tuple(jax.ShapeDtypeStruct((r, 512), jnp.float32) for r in rows),
        in_specs=[VMEM] * len(arrays),
        out_specs=(VMEM,) * len(jobs),
        compiler_params=pltpu.CompilerParams(vmem_limit_bytes=LIMIT),
        cost_estimate=pl.CostEstimate(
            flops=sum(rows) * 2 * 512 * BLOCK * 128 * 2, bytes_accessed=1 << 16, transcendentals=0
        ),
    )(*arrays)


def user_rows(parts, groups, caps=None, items=(), names=()):
    n = len(groups)
    used = [(v, names_) for v, names_ in parts if any(name[0] in groups for name in names_)]
    todo = [] if caps is None else [caps, *items]

    def body(*refs):
        out, rows = refs[-2], refs[-1]
        y = lax.axis_index("y")
        c = lax.axis_index("c")

        def keep(group, block, row):
            dy, other = block
            at = ((y + along(c) * dy + 4) % 4) * 2 + (1 - c if other else c)
            place = (at // 4) * (4 * n) + groups.index(group) * 4 + at % 4
            rows[pl.ds(place, 1), :] = row

        if todo:
            last = refs[len(used)][...]
            for (group, block), iref in zip(names, pieces(refs[len(used) + 1 : -2], BLOCK)):
                keep(group, block, score_row(last, iref))
        for ref, (_, names_) in zip(refs, used):
            for r, (group, block) in enumerate(names_):
                if group in groups:
                    keep(group, block, ref[r : r + 1, :])
        by_user = jnp.max(rows[...].T.reshape(64, 8, 8 * n), axis=1)
        halves = jnp.concatenate([by_user[:, : 4 * n], by_user[:, 4 * n :]], axis=0)
        out[...] = halves.T.reshape(n, 4, 128)

    return pl.pallas_call(
        body,
        out_shape=jax.ShapeDtypeStruct((n, 4, 128), jnp.float32),
        in_specs=[VMEM] * (len(used) + len(todo)),
        out_specs=VMEM,
        compiler_params=pltpu.CompilerParams(vmem_limit_bytes=LIMIT),
        scratch_shapes=[pltpu.VMEM((8 * n, 512), jnp.float32)],
        cost_estimate=pl.CostEstimate(
            flops=(1 + 8 * len(names)) * 512 * BLOCK * 128, bytes_accessed=1 << 16, transcendentals=0
        ),
    )(*[v for v, _ in used], *todo)


def pause():
    def body(out):
        out[...] = jnp.zeros((8, 128), jnp.float32)

    return pl.pallas_call(
        body,
        out_shape=jax.ShapeDtypeStruct((8, 128), jnp.float32),
        out_specs=VMEM,
        compiler_params=pltpu.CompilerParams(vmem_limit_bytes=LIMIT),
        cost_estimate=pl.CostEstimate(flops=1 << 31, bytes_accessed=4096, transcendentals=0),
    )()


def join(first, second, idle):
    def body(first_ref, second_ref, idle_ref, out):
        out[:512, :] = first_ref[...]
        out[512:, :] = second_ref[...]

    return pl.pallas_call(
        body,
        out_shape=jax.ShapeDtypeStruct((1024, 128), jnp.bfloat16),
        in_specs=[VMEM, VMEM, VMEM],
        out_specs=VMEM,
        compiler_params=pltpu.CompilerParams(vmem_limit_bytes=LIMIT),
    )(first, second, idle)


def by_owner(kept, swapped):
    def body(kept_ref, swapped_ref, out):
        z = lax.axis_index("z")
        step = along(lax.axis_index("c"))
        for x in range(SIZES[0]):
            for i, (dz, _) in enumerate(KEPT):
                out[x * 8 + (z + step * dz + 8) % 8] = kept_ref[i]
            for i, (dz, _) in enumerate(SWAPPED):
                out[x * 8 + (z - step * dz + 8) % 8] = swapped_ref[i]

    return pl.pallas_call(
        body,
        out_shape=jax.ShapeDtypeStruct((32, 4, 128), jnp.float32),
        in_specs=[VMEM, VMEM],
        out_specs=VMEM,
        compiler_params=pltpu.CompilerParams(vmem_limit_bytes=LIMIT),
    )(kept, swapped)


def finish(table):
    def body(table_ref, relative, peak):
        x = lax.axis_index("x")
        top = jnp.max(jnp.max(table_ref[...], axis=0), axis=0, keepdims=True)
        top = jnp.maximum(top[:, :64], top[:, 64:])
        mine = [table_ref[x * 8 + z] for z in range(8)]
        rows = jnp.concatenate([part for m in mine for part in (m[:, :64], m[:, 64:])], axis=0)
        relative[...] = (rows - top).T
        peak[...] = top[0]

    return pl.pallas_call(
        body,
        out_shape=(jax.ShapeDtypeStruct((64, 64), jnp.float32), jax.ShapeDtypeStruct((64,), jnp.float32)),
        in_specs=[VMEM],
        out_specs=(VMEM, VMEM),
        compiler_params=pltpu.CompilerParams(vmem_limit_bytes=LIMIT),
    )(table)


def peaks(capsules, bank):
    own = capsules.reshape(512, 128)
    own_x = to_partner(own)
    bank_x = to_partner(bank)
    idle = pause()
    own_pair = join(own, own_x, idle)
    here, sides, sides_x, far, far_x = [(0, 0), (0, 1)], [(1, 0), (-1, 0)], [(-1, 1), (1, 1)], [(2, 0)], [(2, 1)]
    g0, g1, g2, g3, g4 = [(0, 0)], [(1, 0), (1, 1)], [(2, 0), (2, 1)], [(3, 0), (3, 1)], [(4, 0)]
    parts = []

    def score(*jobs):
        rows = scores(*[(caps, items) for caps, _, items, _ in jobs])
        for row, (_, groups, _, blocks) in zip(rows, jobs):
            parts.append((row, [(g, b) for g in groups for b in blocks]))

    ya = down_y(bank)
    yb = down_y(bank, -1)
    z1 = down_z(own_pair)
    z2 = down_z(own_pair, 2)
    z3 = down_z(z1, 2)
    score(([own], g0, [bank, bank_x], here))
    ya = after(ya, parts[-1][0])
    beside = jnp.concatenate([ya, after(yb, parts[-1][0])], axis=0)
    beside_x = to_partner(beside)
    y2 = down_y(ya)
    y2x = to_partner(y2)
    close, close_names = [bank, bank_x, beside, beside_x], here + sides + sides_x
    score(([own], g0, [beside], sides), ([z1], g1, [bank, bank_x, beside], here + sides))
    score(([own, z1], g0 + g1, [beside_x], sides_x), ([z2], g2, close, close_names))
    far_half = after(z3, parts[-1][0])[:512]
    z4 = down_z(far_half)
    score(([z3], g3, close, close_names), ([own, z1, z2, z3], g0 + g1 + g2 + g3, [y2, y2x], far + far_x))
    rows = user_rows(parts, SWAPPED)
    swapped = to_partner(rows)
    every = [(g4[0], b) for b in close_names + far + far_x]
    kept = user_rows(parts, KEPT, z4, close + [y2, y2x], every)
    table = lax.all_to_all(by_owner(kept, swapped), ("x", "z"), 0, 0, tiled=True)
    return finish(table)


def solution(mesh):
    grid = Mesh(mesh.devices.reshape(SIZES), AXES)
    return jax.shard_map(
        peaks,
        mesh=grid,
        in_specs=(P(("z", "y", "c"), None, None), P(AXES, None)),
        out_specs=(P(("z", "y", "c"), "x"), P(("z", "y", "c"))),
        check_vma=False,
    )
```
